32 devices in a mesh: dp: 2 (over core), ctx: 16 (over z, y, x).
Axes of the slice: x: 2, y: 2, z: 4, core: 2. Of those that a mesh axis runs over, the one named last changes fastest.
Arguments:
- documents: int32 [8192], P(('dp', 'ctx')), parts along dimension 0, may hold values from 0 to 15, never falling along the last dimension, each value on 1 to 2048 neighbouring positions
- queries: bfloat16 [8192, 4096], P(('dp', 'ctx')), parts along dimension 0, may hold values from -6 to 6
- key_projection_rows: bfloat16 [8192, 512], P(('dp', 'ctx')), parts along dimension 0, may hold values from -6 to 6
- value_projection_rows: bfloat16 [8192, 512], P(('dp', 'ctx')), parts along dimension 0, may hold values from -6 to 6
Outputs:
- attended: bfloat16 [8192, 4096], P(('dp', 'ctx')), parts along dimension 0
The draws below stay inside these ranges and needn't reach their ends.
There are 2 independent parts, one for each index of `dp`. The reference program is written for one: setup_inputs(seed, part) draws one part's arguments, and reference() takes and returns one part's arrays. A program takes and returns all parts, laid end to end along the dimension named above; each array names one. Nothing has to cross between parts.
Inputs may be any that keep to these rules, and one draw needn't show every extreme that they name: `documents`: document numbers never fall along the sequence; every number appears; each document has 1 to 2048 tokens and one has exactly 2048.
All inputs are finite; a program needn't handle non-finite values.
Results may differ from the reference program's by a relative error of at most 0.0074.
Values may be sent and summed in bfloat16 or wider, within the bound.
A program may use at most 192 MiB of HBM per device.

```python
import math
import jax
import jax.numpy as jnp
import numpy as np
from jax import lax

HEAD_WIDTH = 128
QUERY_HEADS = 32
KEY_VALUE_HEADS = 4
DOCS = 16
DEVICE_TOKENS = 256
PACKED_TOKENS = 4096
MOST = 2048


def shared_draw(key):
    base = jax.random.fold_in(key, 7)
    key_q, key_matrix, key_pick, key_polarity = jax.random.split(base, 4)
    key_result = jnp.clip(jax.random.normal(key_matrix, (PACKED_TOKENS, KEY_VALUE_HEADS * HEAD_WIDTH), jnp.float32), -6.0, 6.0)
    query_out = jnp.clip(jax.random.normal(key_q, (PACKED_TOKENS, QUERY_HEADS * HEAD_WIDTH), jnp.float32), -6.0, 6.0)
    return (query_out, key_result)


def draw_queries(key, part):
    return shared_draw(key)[0].astype(jnp.bfloat16)


def draw_key_projection_rows(key, part):
    return shared_draw(key)[1].astype(jnp.bfloat16)


def block_levels(rng, dims, cuts, smallest, high):
    def one(position, blocks):
        steps = jax.random.uniform(jax.random.fold_in(jax.random.fold_in(rng, 6), position), (blocks,), jnp.float32, smallest / len(cuts), high / len(cuts))
        return jnp.repeat(jnp.exp(steps), dims[position] // blocks).reshape((-1,) + (1,) * (len(dims) - position - 1))

    level = one(*cuts[0])
    for cut in cuts[1:]:
        level = level * one(*cut)
    return level


def profile(count, total, limit, skew):
    portions = [(1 << 20) // math.isqrt(rank ** skew) + 1 for rank in range(2, count + 1)]
    surplus, given = total - limit - (count - 1), [1] * (count - 1)
    while surplus > 0:
        free = [i for i in range(count - 1) if given[i] < limit]
        mass, left = sum([portions[i] for i in free]), surplus
        for i in free:
            extra = min(limit - given[i], max(1, left * portions[i] // mass), surplus)
            given[i] = given[i] + extra
            surplus = surplus - extra
    return np.array([limit] + given)


def uneven(rng, number_of, total, bound, skew):
    if number_of == 2:
        one = jax.random.randint(rng, (), max(1, total - bound), min(bound, total - 1) + 1)
        return jnp.stack([one, total - one])
    lengths = jnp.asarray(profile(number_of, total, bound, skew), jnp.int32)
    twos = (number_of - 1) // 2
    giver, taker = lengths[1:1 + 2 * twos:2], lengths[2:2 + 2 * twos:2]
    slack = jnp.minimum(giver - 1, bound - taker)
    shifted = jax.random.randint(jax.random.fold_in(rng, 1), (twos,), 0, 1 << 20) % (slack + 1)
    lengths = lengths.at[1:1 + 2 * twos:2].set(giver - shifted).at[2:2 + 2 * twos:2].set(taker + shifted)
    return lengths[jax.random.permutation(jax.random.fold_in(rng, 2), number_of)]


def noise(stream_key, shape, deviation, most, cuts=(), held_as=jnp.bfloat16):
    loudness = block_levels(stream_key, shape, cuts, -0.22, 0.18) if cuts else 1.0
    values = jax.random.normal(stream_key, shape, jnp.float32) * deviation * loudness
    return jnp.minimum(jnp.maximum(values, -most), most).astype(held_as)


def setup_inputs(seed: int = 0, part: int = 0) -> dict:
    streams_of = jax.random.split(jax.random.key(seed), 5)
    part_keys = jax.random.split(jax.random.fold_in(streams_of[4], part), 5)
    documents = jnp.searchsorted(jnp.cumsum(uneven(part_keys[0], DOCS, PACKED_TOKENS, MOST, 2)), jnp.arange(PACKED_TOKENS), side="right").astype(jnp.int32)
    queries = draw_queries(jax.random.fold_in(jax.random.fold_in(streams_of[4], part), 71), part)
    key_projection_rows = draw_key_projection_rows(jax.random.fold_in(jax.random.fold_in(streams_of[4], part), 71), part)
    value_projection_rows = noise(part_keys[3], (PACKED_TOKENS, KEY_VALUE_HEADS * HEAD_WIDTH), 1.0, 6.0, ((0, 16),))
    return dict(documents=documents, queries=queries, key_projection_rows=key_projection_rows, value_projection_rows=value_projection_rows)


def apply_rotary_rows(matrix, document_position, head_count):
    total_row_count = matrix.shape[0]
    head_size = matrix.shape[1] // head_count
    half_dim = head_size // 2
    widened = matrix.astype(jnp.float32).reshape(total_row_count, head_count, head_size)
    inverse = jnp.power(jnp.float32(1000000.0), -2.0 * jnp.arange(half_dim, dtype=jnp.float32) / head_size)
    angles = document_position.astype(jnp.float32)[:, None] * inverse[None, :]
    cosine = jnp.cos(angles)[:, None, :]
    sine_part = jnp.sin(angles)[:, None, :]
    front = widened[..., :half_dim]
    back = widened[..., half_dim:]
    rotated = jnp.concatenate([front * cosine - back * sine_part, back * cosine + front * sine_part], axis=-1)
    return rotated.reshape(total_row_count, head_count * head_size).astype(jnp.bfloat16)


def reference(documents, queries, key_projection_rows, value_projection_rows):
    token_count = documents.shape[0]
    index_all = jnp.arange(token_count, dtype=jnp.int32)
    doc_start = jnp.searchsorted(documents, documents, side="left").astype(jnp.int32)
    document_position = index_all - doc_start
    rotary_queries = apply_rotary_rows(queries, document_position, QUERY_HEADS)
    rotary_keys = apply_rotary_rows(key_projection_rows, document_position, KEY_VALUE_HEADS)
    query_group_width = QUERY_HEADS // KEY_VALUE_HEADS
    covered_rows = MOST + DEVICE_TOKENS
    scaling = HEAD_WIDTH ** -0.5

    def one_block(block_number):
        query_block_begin = (block_number * DEVICE_TOKENS).astype(jnp.int32)
        key_block_begin = jnp.clip(query_block_begin - MOST, 0, token_count - covered_rows).astype(jnp.int32)
        query_tile_block = lax.dynamic_slice_in_dim(rotary_queries, query_block_begin, DEVICE_TOKENS, 0).astype(jnp.float32).reshape(DEVICE_TOKENS, KEY_VALUE_HEADS, query_group_width, HEAD_WIDTH)
        key_tile_block = lax.dynamic_slice_in_dim(rotary_keys, key_block_begin, covered_rows, 0).astype(jnp.float32).reshape(covered_rows, KEY_VALUE_HEADS, HEAD_WIDTH)
        value_tile_block = lax.dynamic_slice_in_dim(value_projection_rows, key_block_begin, covered_rows, 0).astype(jnp.float32).reshape(covered_rows, KEY_VALUE_HEADS, HEAD_WIDTH)
        query_index = query_block_begin + jnp.arange(DEVICE_TOKENS, dtype=jnp.int32)
        key_index = key_block_begin + jnp.arange(covered_rows, dtype=jnp.int32)
        starts = lax.dynamic_slice_in_dim(doc_start, query_block_begin, DEVICE_TOKENS, 0)
        allowed = (key_index[None, :] <= query_index[:, None]) & (key_index[None, :] >= starts[:, None])
        scores = jnp.einsum("qkgd,nkd->kgqn", query_tile_block, key_tile_block) * scaling
        scores = jnp.where(allowed, scores, jnp.float32(-1e30))
        top_score = jnp.max(scores, axis=-1, keepdims=True)
        weights = jnp.where(allowed, jnp.exp(scores - top_score), jnp.float32(0.0))
        denominator = jnp.sum(weights, axis=-1)
        mixed = jnp.einsum("kgqn,nkd->kgqd", weights.astype(jnp.bfloat16).astype(jnp.float32), value_tile_block)
        mixed = mixed / denominator[..., None]
        return mixed.transpose(2, 0, 1, 3).reshape(DEVICE_TOKENS, QUERY_HEADS * HEAD_WIDTH).astype(jnp.bfloat16)

    result = lax.map(one_block, jnp.arange(token_count // DEVICE_TOKENS, dtype=jnp.int32))
    return result.reshape(token_count, QUERY_HEADS * HEAD_WIDTH)
```

```python
import functools

import jax
import jax.numpy as jnp
from jax import lax
from jax.experimental import pallas as pl
from jax.experimental.pallas import tpu as pltpu
from jax.sharding import PartitionSpec as P

HEAD_WIDTH = 128
QUERY_HEADS = 32
KEY_VALUE_HEADS = 4
GROUP_HEADS = QUERY_HEADS // KEY_VALUE_HEADS
MOST = 2048
GROUP = 4
DOC_ROWS = 16
UNROLL = 2
KV_WIDTH = KEY_VALUE_HEADS * HEAD_WIDTH
LOG2E = 1.4426950408889634
MASKED = -1e30
LOWEST = -1e29


def turn(x, cosine, sine):
    x = x.astype(jnp.float32)
    return x * cosine + pltpu.roll(x, HEAD_WIDTH // 2, 1) * sine


def pack_kernel(k_ref, v_ref, doc_ref, cos_ref, sin_ref, out_ref):
    rows = k_ref.shape[0]
    cosine, sine = cos_ref[...], sin_ref[...]
    for head in range(KEY_VALUE_HEADS):
        lanes = slice(head * HEAD_WIDTH, (head + 1) * HEAD_WIDTH)
        out_ref[:rows, lanes] = turn(k_ref[:, lanes], cosine, sine).astype(jnp.bfloat16)
    out_ref[:rows, KV_WIDTH:] = v_ref[...]
    out_ref[rows:, :] = jnp.zeros((DOC_ROWS, 2 * KV_WIDTH), jnp.bfloat16)
    out_ref[rows:, :rows] = doc_ref[...]


def turn_queries_kernel(q_ref, cos_ref, sin_ref, out_ref):
    rows = q_ref.shape[0]
    factor = HEAD_WIDTH ** -0.5 * LOG2E
    cosine, sine = cos_ref[...] * factor, sin_ref[...] * factor
    for head in range(GROUP_HEADS):
        lanes = slice(head * HEAD_WIDTH, (head + 1) * HEAD_WIDTH)
        turned = turn(q_ref[:, lanes], cosine, sine).astype(jnp.bfloat16)
        out_ref[0, head * rows:(head + 1) * rows, :] = turned


def attend_kernel(parts, own, first, last, *refs):
    refs = list(refs)
    q_ref, qdoc_ref = refs[:2]
    kv = [refs[2 + 3 * i:5 + 3 * i] for i in range(parts)]
    refs = refs[2 + 3 * parts:]
    if not first:
        acc_in, ml_in = refs[:2]
        refs = refs[2:]
    if last:
        out_ref, acc_ref, ml_ref = refs
    else:
        acc_ref, ml_ref = refs
    rows = qdoc_ref.shape[0]
    half = HEAD_WIDTH // 2

    def put_ml(where, top, total):
        lane = lax.broadcasted_iota(jnp.int32, (rows, HEAD_WIDTH), 1)
        ml_ref[0, where, :] = jnp.where(lane < half, top, total)

    if not first:
        acc_ref[...] = acc_in[...]
        ml_ref[...] = ml_in[...]

    qdoc = qdoc_ref[...]
    q_low, q_high = jnp.min(qdoc), jnp.max(qdoc)

    def update(k_ref, v_ref, mask, fresh):
        k, v = k_ref[...], v_ref[...]
        def one(head):
            where = pl.ds(pl.multiple_of(head * rows, rows), rows)
            s = lax.dot_general(
                q_ref[0, where, :], k, (((1,), (1,)), ((), ())),
                preferred_element_type=jnp.float32,
            )
            if mask is not None:
                s = jnp.where(mask, s, MASKED)
            top = jnp.max(s, axis=1, keepdims=True)
            if not fresh:
                top_before = ml_ref[0, where, 0:1]
                top = jnp.maximum(top, top_before)
            w = jnp.exp2(s - top)
            total = jnp.sum(w, axis=1, keepdims=True)
            product = jnp.dot(w.astype(jnp.bfloat16), v, preferred_element_type=jnp.float32)
            if not fresh:
                shrink = jnp.exp2(top_before - top)
                total = total + ml_ref[0, where, half:half + 1] * shrink
                product = product + acc_ref[0, where, :] * shrink
            acc_ref[0, where, :] = product
            put_ml(where, top, total)

        def some(step, carry):
            for inner in range(UNROLL):
                one(step * UNROLL + inner)
            return carry

        lax.fori_loop(0, GROUP_HEADS // UNROLL, some, 0)

    for index, (k_ref, v_ref, kdoc_ref) in enumerate(kv):
        kdoc = kdoc_ref[0:1, :].astype(jnp.float32)
        if own and index == 0:
            shape = (rows, rows)
            mask = (kdoc == qdoc) & (
                lax.broadcasted_iota(jnp.int32, shape, 1)
                <= lax.broadcasted_iota(jnp.int32, shape, 0)
            )
            update(k_ref, v_ref, mask, True)
            continue
        k_low, k_high = jnp.min(kdoc), jnp.max(kdoc)
        whole = k_low == q_high

        @pl.when(whole)
        def _(k_ref=k_ref, v_ref=v_ref):
            update(k_ref, v_ref, None, False)

        @pl.when((k_high == q_low) & jnp.logical_not(whole))
        def _(k_ref=k_ref, v_ref=v_ref, kdoc=kdoc):
            update(k_ref, v_ref, kdoc == qdoc, False)

    if last:
        for head in range(GROUP_HEADS):
            where = slice(head * rows, (head + 1) * rows)
            out_ref[:, head * HEAD_WIDTH:(head + 1) * HEAD_WIDTH] = (
                acc_ref[0, where, :] / ml_ref[0, where, half:half + 1]
            ).astype(jnp.bfloat16)


def attend(rq, qdoc, blocks, state, own, last):
    rows = qdoc.shape[0]
    wide = GROUP_HEADS * rows
    heads = KEY_VALUE_HEADS
    q_spec = pl.BlockSpec((1, wide, HEAD_WIDTH), lambda g: (g, 0, 0))
    in_specs = [q_spec, pl.BlockSpec((rows, 1), lambda g: (0, 0))]
    args = [rq, qdoc]
    for block in blocks:
        in_specs += [
            pl.BlockSpec((rows, HEAD_WIDTH), lambda g: (0, g)),
            pl.BlockSpec((rows, HEAD_WIDTH), lambda g: (0, heads + g)),
            pl.BlockSpec((DOC_ROWS, rows), lambda g: (rows // DOC_ROWS, 0)),
        ]
        args += [block] * 3
    scratch = []
    if state is not None:
        in_specs += [q_spec, q_spec]
        args += list(state)
    if last:
        out_shape = jax.ShapeDtypeStruct((rows, QUERY_HEADS * HEAD_WIDTH), jnp.bfloat16)
        out_specs = pl.BlockSpec((rows, GROUP_HEADS * HEAD_WIDTH), lambda g: (0, g))
        scratch = [pltpu.VMEM((1, wide, HEAD_WIDTH), jnp.float32)] * 2
    else:
        out_shape = [jax.ShapeDtypeStruct((heads, wide, HEAD_WIDTH), jnp.float32)] * 2
        out_specs = [q_spec, q_spec]
    flops = 4 * rows * rows * QUERY_HEADS * HEAD_WIDTH * len(blocks)
    return pl.pallas_call(
        functools.partial(attend_kernel, len(blocks), own, state is None, last),
        grid=(heads,),
        in_specs=in_specs,
        out_specs=out_specs,
        out_shape=out_shape,
        scratch_shapes=scratch,
        compiler_params=pltpu.CompilerParams(
            dimension_semantics=("arbitrary",), vmem_limit_bytes=48 * 1024 * 1024
        ),
        cost_estimate=pl.CostEstimate(
            flops=4 * flops, bytes_accessed=8 * 1024 * 1024,
            transcendentals=rows * rows * QUERY_HEADS * len(blocks),
        ),
    )(*args)


def shards(documents, queries, key_rows, value_rows):
    rows = documents.shape[0]
    count = lax.axis_size("ctx")
    position = lax.axis_index("ctx") * rows + jnp.arange(rows, dtype=jnp.int32)
    lane = jnp.arange(HEAD_WIDTH, dtype=jnp.int32)
    half = HEAD_WIDTH // 2
    inverse = jnp.power(
        jnp.float32(1000000.0), -2.0 * (lane % half).astype(jnp.float32) / HEAD_WIDTH
    )
    angles = position.astype(jnp.float32)[:, None] * inverse[None, :]
    cosine = jnp.cos(angles)
    sine = jnp.sin(angles) * jnp.where(lane < half, -1.0, 1.0)[None, :]
    marks = (documents + 1).astype(jnp.float32)
    qdoc = marks[:, None]
    kdoc = jnp.broadcast_to(marks.astype(jnp.bfloat16)[None, :], (DOC_ROWS, rows))

    packed = pl.pallas_call(
        pack_kernel,
        out_shape=jax.ShapeDtypeStruct((rows + DOC_ROWS, 2 * KV_WIDTH), jnp.bfloat16),
    )(key_rows, value_rows, kdoc, cosine, sine)

    table = pl.BlockSpec((rows, HEAD_WIDTH), lambda g: (0, 0))
    rq = pl.pallas_call(
        turn_queries_kernel,
        grid=(KEY_VALUE_HEADS,),
        in_specs=[pl.BlockSpec((rows, GROUP_HEADS * HEAD_WIDTH), lambda g: (0, g)), table, table],
        out_specs=pl.BlockSpec((1, GROUP_HEADS * rows, HEAD_WIDTH), lambda g: (g, 0, 0)),
        out_shape=jax.ShapeDtypeStruct(
            (KEY_VALUE_HEADS, GROUP_HEADS * rows, HEAD_WIDTH), jnp.bfloat16
        ),
        cost_estimate=pl.CostEstimate(
            flops=1 << 28, bytes_accessed=4 * 1024 * 1024, transcendentals=0
        ),
    )(queries, cosine, sine)

    reach = -(-(MOST - 1) // rows)
    hops = -(-reach // GROUP)

    def within(block, bit, hop):
        pairs = []
        for target in range(count):
            member = target % GROUP
            source = target - member + (member ^ bit)
            distance = hop * GROUP + target - source
            if 0 < distance <= reach and source - hop * GROUP >= 0:
                pairs.append((source, target))
        return lax.ppermute(block, "ctx", pairs)

    def onward(block, hop):
        pairs = [(s, s + GROUP) for s in range((hop - 1) * GROUP, count - GROUP)]
        return lax.ppermute(block, "ctx", pairs)

    column = packed
    state = None
    for hop in range(hops + 1):
        if hop:
            column = onward(column, hop)
        blocks = [column] + [within(column, bit, hop) for bit in range(1, GROUP)]
        if hop == 0:
            state = attend(rq, qdoc, blocks, None, True, hops == 0)
        else:
            state = attend(rq, qdoc, blocks, state, False, hop == hops)
    return state


def solution(mesh):
    in_specs = (
        P(("dp", "ctx")),
        P(("dp", "ctx"), None),
        P(("dp", "ctx"), None),
        P(("dp", "ctx"), None),
    )
    out_specs = P(("dp", "ctx"), None)
    return jax.shard_map(shards, mesh=mesh, in_specs=in_specs, out_specs=out_specs, check_vma=False)
```

```python
import functools

import jax
import jax.numpy as jnp
from jax import lax
from jax.experimental import pallas as pl
from jax.experimental.pallas import tpu as pltpu
from jax.sharding import PartitionSpec as P

HEAD_WIDTH = 128
QUERY_HEADS = 32
KEY_VALUE_HEADS = 4
GROUP_HEADS = QUERY_HEADS // KEY_VALUE_HEADS
MOST = 2048
GROUP = 4
DOC_ROWS = 16
UNROLL = 4
KV_WIDTH = KEY_VALUE_HEADS * HEAD_WIDTH
LOG2E = 1.4426950408889634
MASKED = -1e30
LOWEST = -1e29


def turn(x, cosine, sine):
    x = x.astype(jnp.float32)
    return x * cosine + pltpu.roll(x, HEAD_WIDTH // 2, 1) * sine


def pack_kernel(k_ref, v_ref, doc_ref, cos_ref, sin_ref, out_ref):
    rows = k_ref.shape[0]
    cosine, sine = cos_ref[...], sin_ref[...]
    for head in range(KEY_VALUE_HEADS):
        lanes = slice(head * HEAD_WIDTH, (head + 1) * HEAD_WIDTH)
        out_ref[:rows, lanes] = turn(k_ref[:, lanes], cosine, sine).astype(jnp.bfloat16)
    per_band = KV_WIDTH // rows
    for head in range(KEY_VALUE_HEADS):
        lanes = slice(head * HEAD_WIDTH, (head + 1) * HEAD_WIDTH)
        band, place = head // per_band, KV_WIDTH + head % per_band * rows
        out_ref[band * HEAD_WIDTH:(band + 1) * HEAD_WIDTH, place:place + rows] = (
            v_ref[:, lanes].astype(jnp.float32).T.astype(jnp.bfloat16)
        )
    out_ref[rows:, :] = jnp.zeros((DOC_ROWS, 2 * KV_WIDTH), jnp.bfloat16)
    out_ref[rows:, :rows] = doc_ref[...]


def turn_queries_kernel(q_ref, cos_ref, sin_ref, out_ref):
    rows = q_ref.shape[0]
    factor = HEAD_WIDTH ** -0.5 * LOG2E
    cosine, sine = cos_ref[...] * factor, sin_ref[...] * factor
    for head in range(GROUP_HEADS):
        lanes = slice(head * HEAD_WIDTH, (head + 1) * HEAD_WIDTH)
        turned = turn(q_ref[:, lanes], cosine, sine).astype(jnp.bfloat16)
        out_ref[0, head * rows:(head + 1) * rows, :] = turned


def attend_kernel(parts, own, first, last, *refs):
    refs = list(refs)
    q_ref, qdoc_ref = refs[:2]
    kv = [refs[2 + 3 * i:5 + 3 * i] for i in range(parts)]
    refs = refs[2 + 3 * parts:]
    if not first:
        acc_in, ml_in = refs[:2]
        refs = refs[2:]
    if last:
        out_ref, acc_ref, ml_ref = refs
    else:
        acc_ref, ml_ref = refs
    rows = qdoc_ref.shape[1]

    if not first:
        acc_ref[...] = acc_in[...]
        ml_ref[...] = ml_in[...]

    qdoc = qdoc_ref[...]
    q_low, q_high = jnp.min(qdoc), jnp.max(qdoc)

    def update(k_ref, vt_ref, mask, fresh):
        k, vt = k_ref[...], vt_ref[...]

        def some(step, carry):
            heads = [step * UNROLL + inner for inner in range(UNROLL)]
            spots = [pl.ds(pl.multiple_of(h * HEAD_WIDTH, HEAD_WIDTH), HEAD_WIDTH) for h in heads]
            before = [None] * UNROLL
            if not fresh:
                before = [
                    (
                        ml_ref[0, pl.ds(h, 1), :],
                        ml_ref[0, pl.ds(GROUP_HEADS + h, 1), :],
                        acc_ref[0, spot, :],
                    )
                    for h, spot in zip(heads, spots)
                ]
            scores = [
                lax.dot_general(
                    k, q_ref[0, pl.ds(pl.multiple_of(h * rows, rows), rows), :],
                    (((1,), (1,)), ((), ())), preferred_element_type=jnp.float32,
                )
                for h in heads
            ]
            results = []
            for s, old in zip(scores, before):
                if mask is not None:
                    s = jnp.where(mask, s, MASKED)
                top = jnp.maximum(jnp.max(s, axis=0, keepdims=True), LOWEST)
                if not fresh:
                    top = jnp.maximum(top, old[0])
                w = jnp.exp2(s - top)
                total = jnp.sum(w, axis=0, keepdims=True)
                product = jnp.dot(vt, w.astype(jnp.bfloat16), preferred_element_type=jnp.float32)
                if not fresh:
                    shrink = jnp.exp2(old[0] - top)
                    total = total + old[1] * shrink
                    product = product + old[2] * shrink
                results.append((top, total, product))
            for h, spot, (top, total, product) in zip(heads, spots, results):
                ml_ref[0, pl.ds(h, 1), :] = top
                ml_ref[0, pl.ds(GROUP_HEADS + h, 1), :] = total
                acc_ref[0, spot, :] = product
            return carry

        lax.fori_loop(0, GROUP_HEADS // UNROLL, some, 0)

    for index, (k_ref, vt_ref, kdoc_ref) in enumerate(kv):
        kdoc = kdoc_ref[0:1, :].astype(jnp.float32)

        def same(kdoc=kdoc):
            column = jnp.broadcast_to(kdoc, (HEAD_WIDTH, rows)).T
            return jnp.concatenate([column] * (rows // HEAD_WIDTH), axis=1) == qdoc

        if own and index == 0:
            shape = (rows, rows)
            mask = same() & (
                lax.broadcasted_iota(jnp.int32, shape, 0)
                <= lax.broadcasted_iota(jnp.int32, shape, 1)
            )
            update(k_ref, vt_ref, mask, True)
            continue
        k_low, k_high = jnp.min(kdoc), jnp.max(kdoc)
        whole = k_low == q_high

        @pl.when(whole)
        def _(k_ref=k_ref, vt_ref=vt_ref):
            update(k_ref, vt_ref, None, False)

        @pl.when((k_high == q_low) & jnp.logical_not(whole))
        def _(k_ref=k_ref, vt_ref=vt_ref, same=same):
            update(k_ref, vt_ref, same(), False)

    if last:
        for head in range(GROUP_HEADS):
            spot = slice(head * HEAD_WIDTH, (head + 1) * HEAD_WIDTH)
            total = ml_ref[0, GROUP_HEADS + head:GROUP_HEADS + head + 1, :]
            out_ref[:, spot] = (acc_ref[0, spot, :] / total).T.astype(jnp.bfloat16)


def attend(rq, qdoc, blocks, state, own, last):
    rows = qdoc.shape[1]
    wide = GROUP_HEADS * rows
    heads = KEY_VALUE_HEADS
    per_band = KV_WIDTH // rows
    acc_shape, ml_shape = (GROUP_HEADS * HEAD_WIDTH, rows), (2 * GROUP_HEADS, rows)
    state_specs = [
        pl.BlockSpec((1,) + shape, lambda g: (g, 0, 0)) for shape in (acc_shape, ml_shape)
    ]
    q_spec = pl.BlockSpec((1, wide, HEAD_WIDTH), lambda g: (g, 0, 0))
    in_specs = [q_spec, pl.BlockSpec((1, rows), lambda g: (0, 0))]
    args = [rq, qdoc]
    for block in blocks:
        in_specs += [
            pl.BlockSpec((rows, HEAD_WIDTH), lambda g: (0, g)),
            pl.BlockSpec((HEAD_WIDTH, rows), lambda g: (g // per_band, KV_WIDTH // rows + g % per_band)),
            pl.BlockSpec((DOC_ROWS, rows), lambda g: (rows // DOC_ROWS, 0)),
        ]
        args += [block] * 3
    scratch = []
    if state is not None:
        in_specs += state_specs
        args += list(state)
    if last:
        out_shape = jax.ShapeDtypeStruct((rows, QUERY_HEADS * HEAD_WIDTH), jnp.bfloat16)
        out_specs = pl.BlockSpec((rows, GROUP_HEADS * HEAD_WIDTH), lambda g: (0, g))
        scratch = [pltpu.VMEM((1,) + shape, jnp.float32) for shape in (acc_shape, ml_shape)]
    else:
        out_shape = [
            jax.ShapeDtypeStruct((heads,) + shape, jnp.float32) for shape in (acc_shape, ml_shape)
        ]
        out_specs = state_specs
    flops = 4 * rows * rows * QUERY_HEADS * HEAD_WIDTH * len(blocks)
    return pl.pallas_call(
        functools.partial(attend_kernel, len(blocks), own, state is None, last),
        grid=(heads,),
        in_specs=in_specs,
        out_specs=out_specs,
        out_shape=out_shape,
        scratch_shapes=scratch,
        compiler_params=pltpu.CompilerParams(
            dimension_semantics=("arbitrary",), vmem_limit_bytes=48 * 1024 * 1024
        ),
        cost_estimate=pl.CostEstimate(
            flops=4 * flops, bytes_accessed=8 * 1024 * 1024,
            transcendentals=rows * rows * QUERY_HEADS * len(blocks),
        ),
    )(*args)


def shards(documents, queries, key_rows, value_rows):
    rows = documents.shape[0]
    count = lax.axis_size("ctx")
    position = lax.axis_index("ctx") * rows + jnp.arange(rows, dtype=jnp.int32)
    lane = jnp.arange(HEAD_WIDTH, dtype=jnp.int32)
    half = HEAD_WIDTH // 2
    inverse = jnp.power(
        jnp.float32(1000000.0), -2.0 * (lane % half).astype(jnp.float32) / HEAD_WIDTH
    )
    angles = position.astype(jnp.float32)[:, None] * inverse[None, :]
    cosine = jnp.cos(angles)
    sine = jnp.sin(angles) * jnp.where(lane < half, -1.0, 1.0)[None, :]
    marks = (documents + 1).astype(jnp.float32)
    qdoc = marks[None, :]
    kdoc = jnp.broadcast_to(marks.astype(jnp.bfloat16)[None, :], (DOC_ROWS, rows))

    packed = pl.pallas_call(
        pack_kernel,
        out_shape=jax.ShapeDtypeStruct((rows + DOC_ROWS, 2 * KV_WIDTH), jnp.bfloat16),
    )(key_rows, value_rows, kdoc, cosine, sine)

    table = pl.BlockSpec((rows, HEAD_WIDTH), lambda g: (0, 0))
    rq = pl.pallas_call(
        turn_queries_kernel,
        grid=(KEY_VALUE_HEADS,),
        in_specs=[pl.BlockSpec((rows, GROUP_HEADS * HEAD_WIDTH), lambda g: (0, g)), table, table],
        out_specs=pl.BlockSpec((1, GROUP_HEADS * rows, HEAD_WIDTH), lambda g: (g, 0, 0)),
        out_shape=jax.ShapeDtypeStruct(
            (KEY_VALUE_HEADS, GROUP_HEADS * rows, HEAD_WIDTH), jnp.bfloat16
        ),
        cost_estimate=pl.CostEstimate(
            flops=1 << 28, bytes_accessed=4 * 1024 * 1024, transcendentals=0
        ),
    )(queries, cosine, sine)

    reach = -(-(MOST - 1) // rows)
    hops = -(-reach // GROUP)

    def within(block, bit, hop):
        pairs = []
        for target in range(count):
            member = target % GROUP
            source = target - member + (member ^ bit)
            distance = hop * GROUP + target - source
            if 0 < distance <= reach and source - hop * GROUP >= 0:
                pairs.append((source, target))
        return lax.ppermute(block, "ctx", pairs)

    def onward(block, hop):
        pairs = [(s, s + GROUP) for s in range((hop - 1) * GROUP, count - GROUP)]
        return lax.ppermute(block, "ctx", pairs)

    column = packed
    state = None
    for hop in range(hops + 1):
        if hop:
            column = onward(column, hop)
        blocks = [column] + [within(column, bit, hop) for bit in range(1, GROUP)]
        if hop == 0:
            state = attend(rq, qdoc, blocks, None, True, hops == 0)
        else:
            state = attend(rq, qdoc, blocks, state, False, hop == hops)
    return state


def solution(mesh):
    in_specs = (
        P(("dp", "ctx")),
        P(("dp", "ctx"), None),
        P(("dp", "ctx"), None),
        P(("dp", "ctx"), None),
    )
    out_specs = P(("dp", "ctx"), None)
    return jax.shard_map(shards, mesh=mesh, in_specs=in_specs, out_specs=out_specs, check_vma=False)
```

```python
import functools

import jax
import jax.numpy as jnp
from jax import lax
from jax.experimental import pallas as pl
from jax.experimental.pallas import tpu as pltpu
from jax.sharding import PartitionSpec as P

HEAD_WIDTH = 128
QUERY_HEADS = 32
KEY_VALUE_HEADS = 4
GROUP_HEADS = QUERY_HEADS // KEY_VALUE_HEADS
MOST = 2048
GROUP = 4
DOC_ROWS = 16
UNROLL = 4
KV_WIDTH = KEY_VALUE_HEADS * HEAD_WIDTH
LOG2E = 1.4426950408889634
MASKED = -1e30
LOWEST = -1e29


def turn(x, cosine, sine):
    x = x.astype(jnp.float32)
    return x * cosine + pltpu.roll(x, HEAD_WIDTH // 2, 1) * sine


def pack_kernel(k_ref, v_ref, doc_ref, cos_ref, sin_ref, out_ref):
    rows = k_ref.shape[0]
    cosine, sine = cos_ref[...], sin_ref[...]
    for head in range(KEY_VALUE_HEADS):
        lanes = slice(head * HEAD_WIDTH, (head + 1) * HEAD_WIDTH)
        out_ref[:rows, lanes] = turn(k_ref[:, lanes], cosine, sine).astype(jnp.bfloat16)
    per_band = KV_WIDTH // rows
    for head in range(KEY_VALUE_HEADS):
        lanes = slice(head * HEAD_WIDTH, (head + 1) * HEAD_WIDTH)
        band, place = head // per_band, KV_WIDTH + head % per_band * rows
        out_ref[band * HEAD_WIDTH:(band + 1) * HEAD_WIDTH, place:place + rows] = (
            v_ref[:, lanes].astype(jnp.float32).T.astype(jnp.bfloat16)
        )
    out_ref[rows:, :] = jnp.zeros((DOC_ROWS, 2 * KV_WIDTH), jnp.bfloat16)
    out_ref[rows:, :rows] = doc_ref[...]


def turn_queries_kernel(q_ref, cos_ref, sin_ref, out_ref):
    rows = q_ref.shape[0]
    factor = HEAD_WIDTH ** -0.5 * LOG2E
    cosine, sine = cos_ref[...] * factor, sin_ref[...] * factor
    for head in range(GROUP_HEADS):
        lanes = slice(head * HEAD_WIDTH, (head + 1) * HEAD_WIDTH)
        turned = turn(q_ref[:, lanes], cosine, sine).astype(jnp.bfloat16)
        out_ref[0, head * rows:(head + 1) * rows, :] = turned


def attend_kernel(parts, own, first, last, *refs):
    refs = list(refs)
    q_ref, qdoc_ref = refs[:2]
    kv = [refs[2 + 3 * i:5 + 3 * i] for i in range(parts)]
    refs = refs[2 + 3 * parts:]
    if not first:
        acc_in, ml_in = refs[:2]
        refs = refs[2:]
    if last:
        out_ref, acc_ref, ml_ref = refs
    else:
        acc_ref, ml_ref = refs
    rows = qdoc_ref.shape[1]

    if not first:
        acc_ref[...] = acc_in[...]
        ml_ref[...] = ml_in[...]

    qdoc = qdoc_ref[...]
    q_low, q_high = jnp.min(qdoc), jnp.max(qdoc)

    def update(k_ref, vt_ref, mask, fresh):
        k, vt = k_ref[...], vt_ref[...]

        def some(step, carry):
            heads = [step * UNROLL + inner for inner in range(UNROLL)]
            spots = [pl.ds(pl.multiple_of(h * HEAD_WIDTH, HEAD_WIDTH), HEAD_WIDTH) for h in heads]
            before = [None] * UNROLL
            if not fresh:
                before = [
                    (
                        ml_ref[0, pl.ds(h, 1), :],
                        ml_ref[0, pl.ds(GROUP_HEADS + h, 1), :],
                        acc_ref[0, spot, :],
                    )
                    for h, spot in zip(heads, spots)
                ]
            def score(h):
                return lax.dot_general(
                    k, q_ref[0, pl.ds(pl.multiple_of(h * rows, rows), rows), :],
                    (((1,), (1,)), ((), ())), preferred_element_type=jnp.float32,
                )

            scores = [score(h) for h in heads]
            results = []
            for s, old in zip(scores, before):
                if mask is not None:
                    s = jnp.where(mask, s, MASKED)
                top = jnp.maximum(jnp.max(s, axis=0, keepdims=True), LOWEST)
                if not fresh:
                    top = jnp.maximum(top, old[0])
                w = jnp.exp2(s - top)
                total = jnp.sum(w, axis=0, keepdims=True)
                product = jnp.dot(vt, w.astype(jnp.bfloat16), preferred_element_type=jnp.float32)
                if not fresh:
                    shrink = jnp.exp2(old[0] - top)
                    total = total + old[1] * shrink
                    product = product + old[2] * shrink
                results.append((top, total, product))
            for h, spot, (top, total, product) in zip(heads, spots, results):
                ml_ref[0, pl.ds(h, 1), :] = top
                ml_ref[0, pl.ds(GROUP_HEADS + h, 1), :] = total
                acc_ref[0, spot, :] = product
            return carry

        lax.fori_loop(0, GROUP_HEADS // UNROLL, some, 0)

    for index, (k_ref, vt_ref, kdoc_ref) in enumerate(kv):
        kdoc = kdoc_ref[0:1, :].astype(jnp.float32)

        def same(kdoc=kdoc):
            column = jnp.broadcast_to(kdoc, (HEAD_WIDTH, rows)).T
            return jnp.concatenate([column] * (rows // HEAD_WIDTH), axis=1) == qdoc

        if own and index == 0:
            shape = (rows, rows)
            mask = same() & (
                lax.broadcasted_iota(jnp.int32, shape, 0)
                <= lax.broadcasted_iota(jnp.int32, shape, 1)
            )
            update(k_ref, vt_ref, mask, True)
            continue
        k_low, k_high = jnp.min(kdoc), jnp.max(kdoc)
        whole = k_low == q_high

        @pl.when(whole)
        def _(k_ref=k_ref, vt_ref=vt_ref):
            update(k_ref, vt_ref, None, False)

        @pl.when((k_high == q_low) & jnp.logical_not(whole))
        def _(k_ref=k_ref, vt_ref=vt_ref, same=same):
            update(k_ref, vt_ref, same(), False)

    if last:
        for head in range(GROUP_HEADS):
            spot = slice(head * HEAD_WIDTH, (head + 1) * HEAD_WIDTH)
            total = ml_ref[0, GROUP_HEADS + head:GROUP_HEADS + head + 1, :]
            out_ref[:, spot] = (acc_ref[0, spot, :] / total).T.astype(jnp.bfloat16)


def attend(rq, qdoc, blocks, state, own, last):
    rows = qdoc.shape[1]
    wide = GROUP_HEADS * rows
    heads = KEY_VALUE_HEADS
    per_band = KV_WIDTH // rows
    acc_shape, ml_shape = (GROUP_HEADS * HEAD_WIDTH, rows), (2 * GROUP_HEADS, rows)
    state_specs = [
        pl.BlockSpec((1,) + shape, lambda g: (g, 0, 0)) for shape in (acc_shape, ml_shape)
    ]
    q_spec = pl.BlockSpec((1, wide, HEAD_WIDTH), lambda g: (g, 0, 0))
    in_specs = [q_spec, pl.BlockSpec((1, rows), lambda g: (0, 0))]
    args = [rq, qdoc]
    for block in blocks:
        in_specs += [
            pl.BlockSpec((rows, HEAD_WIDTH), lambda g: (0, g)),
            pl.BlockSpec((HEAD_WIDTH, rows), lambda g: (g // per_band, KV_WIDTH // rows + g % per_band)),
            pl.BlockSpec((DOC_ROWS, rows), lambda g: (rows // DOC_ROWS, 0)),
        ]
        args += [block] * 3
    scratch = []
    if state is not None:
        in_specs += state_specs
        args += list(state)
    if last:
        out_shape = jax.ShapeDtypeStruct((rows, QUERY_HEADS * HEAD_WIDTH), jnp.bfloat16)
        out_specs = pl.BlockSpec((rows, GROUP_HEADS * HEAD_WIDTH), lambda g: (0, g))
        scratch = [pltpu.VMEM((1,) + shape, jnp.float32) for shape in (acc_shape, ml_shape)]
    else:
        out_shape = [
            jax.ShapeDtypeStruct((heads,) + shape, jnp.float32) for shape in (acc_shape, ml_shape)
        ]
        out_specs = state_specs
    flops = 4 * rows * rows * QUERY_HEADS * HEAD_WIDTH * len(blocks)
    return pl.pallas_call(
        functools.partial(attend_kernel, len(blocks), own, state is None, last),
        grid=(heads,),
        in_specs=in_specs,
        out_specs=out_specs,
        out_shape=out_shape,
        scratch_shapes=scratch,
        compiler_params=pltpu.CompilerParams(
            dimension_semantics=("arbitrary",), vmem_limit_bytes=48 * 1024 * 1024
        ),
        cost_estimate=pl.CostEstimate(
            flops=flops, bytes_accessed=4 * 1024 * 1024,
            transcendentals=rows * rows * QUERY_HEADS * len(blocks),
        ),
    )(*args)


def shards(documents, queries, key_rows, value_rows):
    rows = documents.shape[0]
    count = lax.axis_size("ctx")
    position = lax.axis_index("ctx") * rows + jnp.arange(rows, dtype=jnp.int32)
    lane = jnp.arange(HEAD_WIDTH, dtype=jnp.int32)
    half = HEAD_WIDTH // 2
    inverse = jnp.power(
        jnp.float32(1000000.0), -2.0 * (lane % half).astype(jnp.float32) / HEAD_WIDTH
    )
    angles = position.astype(jnp.float32)[:, None] * inverse[None, :]
    cosine = jnp.cos(angles)
    sine = jnp.sin(angles) * jnp.where(lane < half, -1.0, 1.0)[None, :]
    marks = (documents + 1).astype(jnp.float32)
    qdoc = marks[None, :]
    kdoc = jnp.broadcast_to(marks.astype(jnp.bfloat16)[None, :], (DOC_ROWS, rows))

    packed = pl.pallas_call(
        pack_kernel,
        out_shape=jax.ShapeDtypeStruct((rows + DOC_ROWS, 2 * KV_WIDTH), jnp.bfloat16),
    )(key_rows, value_rows, kdoc, cosine, sine)

    table = pl.BlockSpec((rows, HEAD_WIDTH), lambda g: (0, 0))
    rq = pl.pallas_call(
        turn_queries_kernel,
        grid=(KEY_VALUE_HEADS,),
        in_specs=[pl.BlockSpec((rows, GROUP_HEADS * HEAD_WIDTH), lambda g: (0, g)), table, table],
        out_specs=pl.BlockSpec((1, GROUP_HEADS * rows, HEAD_WIDTH), lambda g: (g, 0, 0)),
        out_shape=jax.ShapeDtypeStruct(
            (KEY_VALUE_HEADS, GROUP_HEADS * rows, HEAD_WIDTH), jnp.bfloat16
        ),
        cost_estimate=pl.CostEstimate(
            flops=1 << 28, bytes_accessed=4 * 1024 * 1024, transcendentals=0
        ),
    )(queries, cosine, sine)

    reach = -(-(MOST - 1) // rows)
    hops = -(-reach // GROUP)

    def within(block, bit, hop):
        pairs = []
        for target in range(count):
            member = target % GROUP
            source = target - member + (member ^ bit)
            distance = hop * GROUP + target - source
            if 0 < distance <= reach and source - hop * GROUP >= 0:
                pairs.append((source, target))
        return lax.ppermute(block, "ctx", pairs)

    def onward(block, hop):
        pairs = [(s, s + GROUP) for s in range((hop - 1) * GROUP, count - GROUP)]
        return lax.ppermute(block, "ctx", pairs)

    members = range(1, GROUP)
    near = [within(packed, bit, 0) for bit in members[:-1]]
    state = attend(rq, qdoc, [packed], None, True, hops == 0)
    first, state = lax.optimization_barrier((onward(packed, 1), state))
    columns = [packed, first]
    for hop in range(2, hops + 1):
        columns.append(onward(columns[-1], hop))
    for hop in range(1, hops):
        blocks = [columns[hop]] + [within(columns[hop], bit, hop) for bit in members]
        state = attend(rq, qdoc, blocks, state, False, False)
    late, _ = lax.optimization_barrier((packed, first))
    near.append(within(late, members[-1], 0))
    far = [within(columns[hops], bit, hops) for bit in members]
    return attend(rq, qdoc, near + [columns[hops]] + far, state, False, True)


def solution(mesh):
    in_specs = (
        P(("dp", "ctx")),
        P(("dp", "ctx"), None),
        P(("dp", "ctx"), None),
        P(("dp", "ctx"), None),
    )
    out_specs = P(("dp", "ctx"), None)
    return jax.shard_map(shards, mesh=mesh, in_specs=in_specs, out_specs=out_specs, check_vma=False)
```
